64 devices in a mesh: dp: 4 (over x, y), sp: 16 (over z, core).
Axes of the slice: x: 2, y: 2, z: 8, core: 2. Of those that a mesh axis runs over, the one named last changes fastest.
The devices are a block of a 4x4x8 slice.
Arguments:
- patches: bfloat16 [8, 4096, 1536], P('dp', 'sp'), parts along dimension 0
- vis_mask: int32 [8, 4096], P('dp', 'sp'), parts along dimension 0
- enc_pos: bfloat16 [16384, 1024], P(('dp', 'sp')), parts along dimension 0
- dec_pos: bfloat16 [16384, 512], P(('dp', 'sp')), parts along dimension 0
- w_pe: bfloat16 [1536, 1024], replicated
- b_pe: bfloat16 [1024], replicated
- enc_qkv: bfloat16 [2, 1024, 3, 16, 64], replicated
- enc_proj: bfloat16 [2, 16, 64, 1024], replicated
- enc_up: bfloat16 [2, 1024, 4096], replicated
- enc_down: bfloat16 [2, 4096, 1024], replicated
- w_ed: bfloat16 [1024, 512], replicated
- mask_token: bfloat16 [512], replicated
- dec_qkv: bfloat16 [2, 512, 3, 16, 32], replicated
- dec_proj: bfloat16 [2, 16, 32, 512], replicated
- dec_up: bfloat16 [2, 512, 2048], replicated
- dec_down: bfloat16 [2, 2048, 512], replicated
- w_out: bfloat16 [512, 1536], replicated
Outputs:
- output: float32 [8, 4096, 1536], P('dp', 'sp'), parts along dimension 0
There are 4 independent parts. The reference program is written for one: setup_inputs(seed, part) draws one part's arguments, and reference() takes and returns one part's arrays. A program takes and returns all parts, laid end to end along the dimension named above; an argument that names none is the same for every part.
All inputs are finite; a program needn't handle non-finite values.
Results may differ from the reference program's by a relative error of at most 0.0157389.
Values are sent between devices in bfloat16 or wider.
A program may use at most 768 MiB of HBM per device.

```python
import jax
import jax.numpy as jnp
from jax import lax

P = 1536
D = 1024
ENC_HEADS = 16
DD = 512
DEC_HEADS = 16
TOK_DEV = 256
SP = 16
KEEP_DIV = 8
CLIPS = 2
LAYERS = 2

SEQ = TOK_DEV * SP
VIS_SHARD = TOK_DEV // KEEP_DIV
VIS_ALL = VIS_SHARD * SP
ENC_HD = D // ENC_HEADS
DEC_HD = DD // DEC_HEADS


def shard_ranks(key):
    return jax.random.permutation(key, TOK_DEV)


def draw_mask(key):
    half_shard = VIS_SHARD // 2
    key_shift, key_pick, key_perm = jax.random.split(key, 3)
    inner_shift = jax.random.randint(key_shift, (CLIPS, SP - 1), -half_shard, half_shard + 1)
    pick_at = jax.random.randint(key_pick, (CLIPS, 1), 1, SP - 2)
    shard_idx = jnp.arange(1, SP)[None, :]
    inner_shift = jnp.where(shard_idx == pick_at, half_shard, inner_shift)
    inner_shift = jnp.where(shard_idx == pick_at + 1, -half_shard, inner_shift)
    inner_shift = jnp.where(shard_idx == pick_at + 2, half_shard, inner_shift)
    edge_zero = jnp.zeros((CLIPS, 1), jnp.int32)
    shift_all = jnp.concatenate([edge_zero, inner_shift, edge_zero], axis=1)
    shard_counts = VIS_SHARD + shift_all[:, 1:] - shift_all[:, :-1]
    tok_ranks = jax.vmap(shard_ranks)(jax.random.split(key_perm, CLIPS * SP))
    tok_ranks = tok_ranks.reshape(CLIPS, SP, TOK_DEV)
    return (tok_ranks < shard_counts[:, :, None]).astype(jnp.int32).reshape(CLIPS, SEQ)


def draw_normal(key, shape, scale):
    return (scale * jax.random.normal(key, shape, jnp.float32)).astype(jnp.bfloat16)


def setup_inputs(seed: int = 0, part: int = 0) -> dict:
    key_shared, key_local = jax.random.split(jax.random.key(seed))
    part_keys = jax.random.split(jax.random.fold_in(key_local, part), 4)
    weight_keys = jax.random.split(key_shared, 13)
    return {
        'patches': draw_normal(part_keys[0], (CLIPS, SEQ, P), 1.0),
        'vis_mask': draw_mask(part_keys[1]),
        'enc_pos': draw_normal(part_keys[2], (SEQ, D), 0.5),
        'dec_pos': draw_normal(part_keys[3], (SEQ, DD), 0.5),
        'w_pe': draw_normal(weight_keys[0], (P, D), P ** -0.5),
        'b_pe': draw_normal(weight_keys[1], (D,), 0.5),
        'enc_qkv': draw_normal(weight_keys[2], (LAYERS, D, 3, ENC_HEADS, ENC_HD), 1.5 * D ** -0.5),
        'enc_proj': draw_normal(weight_keys[3], (LAYERS, ENC_HEADS, ENC_HD, D), D ** -0.5),
        'enc_up': draw_normal(weight_keys[4], (LAYERS, D, 4 * D), D ** -0.5),
        'enc_down': draw_normal(weight_keys[5], (LAYERS, 4 * D, D), (4 * D) ** -0.5),
        'w_ed': draw_normal(weight_keys[6], (D, DD), D ** -0.5),
        'mask_token': draw_normal(weight_keys[7], (DD,), 1.0),
        'dec_qkv': draw_normal(weight_keys[8], (LAYERS, DD, 3, DEC_HEADS, DEC_HD), 1.5 * DD ** -0.5),
        'dec_proj': draw_normal(weight_keys[9], (LAYERS, DEC_HEADS, DEC_HD, DD), DD ** -0.5),
        'dec_up': draw_normal(weight_keys[10], (LAYERS, DD, 4 * DD), DD ** -0.5),
        'dec_down': draw_normal(weight_keys[11], (LAYERS, 4 * DD, DD), (4 * DD) ** -0.5),
        'w_out': draw_normal(weight_keys[12], (DD, P), DD ** -0.5),
    }


def layer_norm(hidden):
    hid_f32 = hidden.astype(jnp.float32)
    centred = hid_f32 - jnp.mean(hid_f32, axis=-1, keepdims=True)
    row_var = jnp.mean(centred * centred, axis=-1, keepdims=True)
    return (centred * lax.rsqrt(row_var + 1e-6)).astype(jnp.bfloat16)


def attend(queries, key_rows, value_rows):
    q_rows, n_heads, head_dim = queries.shape
    keys_f32 = key_rows.astype(jnp.float32)
    values_f32 = value_rows.astype(jnp.float32)

    def one_block(q_block):
        scores = jnp.einsum('qhk,shk->hqs', q_block.astype(jnp.float32), keys_f32) * head_dim ** -0.5
        attn_probs = jax.nn.softmax(scores, axis=-1).astype(jnp.bfloat16)
        return jnp.einsum('hqs,shk->qhk', attn_probs.astype(jnp.float32), values_f32).astype(jnp.bfloat16)

    q_blocks = queries.reshape(SP, q_rows // SP, n_heads, head_dim)
    return lax.map(one_block, q_blocks).reshape(q_rows, n_heads, head_dim)


def block(hidden, w_qkv, w_proj, w_up, w_down):
    proj_qkv = jnp.einsum('nd,dshk->snhk', layer_norm(hidden).astype(jnp.float32), w_qkv.astype(jnp.float32)).astype(jnp.bfloat16)
    attended = attend(proj_qkv[0], proj_qkv[1], proj_qkv[2])
    att_out = jnp.einsum('nhk,hkd->nd', attended.astype(jnp.float32), w_proj.astype(jnp.float32))
    mid_state = (hidden.astype(jnp.float32) + att_out).astype(jnp.bfloat16)
    up_act = jax.nn.gelu(jnp.dot(layer_norm(mid_state), w_up, preferred_element_type=jnp.float32), approximate=False).astype(jnp.bfloat16)
    return (mid_state.astype(jnp.float32) + jnp.dot(up_act, w_down, preferred_element_type=jnp.float32)).astype(jnp.bfloat16)


def run_stack(hidden, w_qkv, w_proj, w_up, w_down):
    def body(carry, layer_w):
        return block(carry, layer_w[0], layer_w[1], layer_w[2], layer_w[3]), None

    final_state, unused = lax.scan(body, hidden, (w_qkv, w_proj, w_up, w_down))
    return final_state


def reference(patches, vis_mask, enc_pos, dec_pos, w_pe, b_pe, enc_qkv, enc_proj, enc_up, enc_down, w_ed, mask_token, dec_qkv, dec_proj, dec_up, dec_down, w_out):
    def one_clip(clip_in):
        clip_patches, visible = clip_in
        vis_idx = jnp.nonzero(visible, size=VIS_ALL)[0]
        embedded = (jnp.dot(clip_patches[vis_idx], w_pe, preferred_element_type=jnp.float32)
                    + b_pe.astype(jnp.float32) + enc_pos[vis_idx].astype(jnp.float32)).astype(jnp.bfloat16)
        encoded = run_stack(embedded, enc_qkv, enc_proj, enc_up, enc_down)
        z_vis = jnp.dot(layer_norm(encoded), w_ed, preferred_element_type=jnp.float32).astype(jnp.bfloat16)
        vis_rank = jnp.clip(jnp.cumsum(visible) - visible, 0, VIS_ALL - 1)
        dec_tok = jnp.where(visible[:, None] == 1, z_vis[vis_rank], mask_token[None, :])
        dec_in = (dec_tok.astype(jnp.float32) + dec_pos.astype(jnp.float32)).astype(jnp.bfloat16)
        decoded = run_stack(dec_in, dec_qkv, dec_proj, dec_up, dec_down)
        return jnp.dot(layer_norm(decoded), w_out, preferred_element_type=jnp.float32)

    return lax.map(one_clip, (patches, vis_mask))
```

```python
import functools

import jax
import jax.numpy as jnp
from jax import lax
from jax.experimental import pallas as pl
from jax.experimental.pallas import tpu as pltpu
from jax.sharding import PartitionSpec as P

KEEP_DIV = 8
PIECES = 2
MESH = pl.DeviceIdType.MESH
LOG2E = 1.4426950408889634
NT = (((1,), (1,)), ((), ()))
TN = (((0,), (0,)), ((), ()))


def layer_norm(hidden):
    hid_f32 = hidden.astype(jnp.float32)
    centred = hid_f32 - jnp.mean(hid_f32, axis=-1, keepdims=True)
    row_var = jnp.mean(centred * centred, axis=-1, keepdims=True)
    return (centred * lax.rsqrt(row_var + 1e-6)).astype(jnp.bfloat16)


def gelu(x):
    return 0.5 * x * (1.0 + lax.erf(x * 0.7071067811865476))


def fdot(lhs, rhs, dims=(((1,), (0,)), ((), ()))):
    return lax.dot_general(lhs, rhs, dims, preferred_element_type=jnp.float32)


def attn_mlp_block(hidden, w_qkv, w_proj, w_up, w_down):
    proj_qkv = jnp.einsum('cnd,dshk->scnhk', layer_norm(hidden), w_qkv, preferred_element_type=jnp.float32).astype(jnp.bfloat16)
    kv_all = lax.all_gather(proj_qkv[1:], 'sp', axis=2, tiled=True)
    scores = jnp.einsum('cqhk,cshk->chqs', proj_qkv[0], kv_all[0], preferred_element_type=jnp.float32) * proj_qkv.shape[-1] ** -0.5
    attn_probs = jax.nn.softmax(scores, axis=-1).astype(jnp.bfloat16)
    attended = jnp.einsum('chqs,cshk->cqhk', attn_probs, kv_all[1], preferred_element_type=jnp.float32).astype(jnp.bfloat16)
    mid_state = (hidden + jnp.einsum('cqhk,hkd->cqd', attended, w_proj, preferred_element_type=jnp.float32)).astype(jnp.bfloat16)
    up_act = jax.nn.gelu(jnp.einsum('cnd,df->cnf', layer_norm(mid_state), w_up, preferred_element_type=jnp.float32), approximate=False).astype(jnp.bfloat16)
    return (mid_state + jnp.einsum('cnf,fd->cnd', up_act, w_down, preferred_element_type=jnp.float32)).astype(jnp.bfloat16)


class RingGather:
    def __init__(self, n_chips, piece_rows, buf, send, recv):
        self.n, self.rows, self.buf, self.send, self.recv = n_chips, piece_rows, buf, send, recv
        me = lax.axis_index('sp')
        size = 2 * n_chips
        self.right = lax.rem(me + 2, size)
        self.left = lax.rem(me + size - 2, size)
        self.mate = me + 1 - 2 * lax.rem(me, 2)
        self.arrivals = PIECES * (n_chips // 2) - 1

    def barrier(self):
        sem = pltpu.get_barrier_semaphore()
        for peer in (self.left, self.right, self.mate):
            pl.semaphore_signal(sem, inc=1, device_id={'sp': peer}, device_id_type=MESH)
        pl.semaphore_wait(sem, 3)

    def copy(self, phase, kind, step, piece):
        if kind == 2:
            src, dst, dst_core, peer = step, step, 1, self.mate
        elif kind == 0:
            src, dst, dst_core, peer = step, step + 1, 0, self.right
        else:
            src, dst, dst_core, peer = lax.rem(self.n - step, self.n), self.n - 1 - step, 0, self.left
        rows = pl.ds(pl.multiple_of(piece * self.rows, self.rows), self.rows)
        return pltpu.make_async_remote_copy(
            src_ref=self.buf.at[phase, src, 0, rows], dst_ref=self.buf.at[phase, dst, dst_core, rows],
            send_sem=self.send.at[phase, kind, step, piece], recv_sem=self.recv.at[phase, kind, step, piece],
            device_id={'sp': peer}, device_id_type=MESH)

    def begin(self, phase):
        for piece in range(PIECES):
            self.copy(phase, 0, 0, piece).start()
            self.copy(phase, 1, 0, PIECES - 1 - piece).start()
            self.copy(phase, 2, 0, piece).start()

    def relay(self, phase, k):
        step = k // PIECES
        p_right = lax.rem(k, PIECES)
        p_left = PIECES - 1 - p_right
        self.copy(phase, 0, step, p_right).wait_recv()
        pl.when(k < self.arrivals - PIECES)(lambda: self.copy(phase, 0, step + 1, p_right).start())
        self.copy(phase, 2, step + 1, p_right).start()
        self.copy(phase, 1, step, p_left).wait_recv()
        pl.when(k < self.arrivals - PIECES)(lambda: self.copy(phase, 1, step + 1, p_left).start())
        self.copy(phase, 2, self.n - 1 - step, p_left).start()

    def finish(self, phase):
        def per_slot(i, carry):
            mate_copy = self.copy(phase, 2, i // PIECES, lax.rem(i, PIECES))
            mate_copy.wait_recv()
            mate_copy.wait_send()
            return carry

        def per_hop(k, carry):
            self.copy(phase, 0, k // PIECES, lax.rem(k, PIECES)).wait_send()
            self.copy(phase, 1, k // PIECES, PIECES - 1 - lax.rem(k, PIECES)).wait_send()
            return carry

        lax.fori_loop(0, PIECES * self.n, per_slot, 0)
        lax.fori_loop(0, self.arrivals, per_hop, 0)


def decoder_kernel(n_chips, n_heads, u_ref, wqkv_hbm, wproj_hbm, wup_hbm, wdown_hbm, state,
                   gath, k_ref, vt_ref, s_ref, m_ref, qm_ref, ot_ref, wqkv, wproj, wup, wdown, send, recv, wsem):
    n_clips, rows, width = u_ref.shape
    n_layers = wproj.shape[0]
    phases = n_layers * n_clips
    head_dim = width // n_heads
    lane_heads = qm_ref.shape[1] // head_dim
    chunk = 2 * rows
    scale = head_dim ** -0.5 * LOG2E
    ring = RingGather(n_chips, rows // PIECES, gath, send, recv)

    weights = [pltpu.make_async_copy(src, dst, wsem.at[i]) for i, (src, dst) in enumerate(
        ((wqkv_hbm, wqkv), (wproj_hbm, wproj), (wup_hbm, wup), (wdown_hbm, wdown)))]
    for copy in weights:
        copy.start()
    for clip in range(n_clips):
        state[clip] = u_ref[clip]
        gath[clip, 0, 0] = layer_norm(u_ref[clip])
    qm_ref[...] = jnp.zeros_like(qm_ref)
    ring.barrier()
    ring.begin(0)
    lax.fori_loop(0, ring.arrivals, lambda k, carry: (ring.relay(0, k), carry)[1], 0)
    for copy in weights:
        copy.wait()

    def scores(head, j, slot, top):
        group = head // lane_heads
        keys = k_ref[j, :, pl.ds(pl.multiple_of(group * qm_ref.shape[1], qm_ref.shape[1]), qm_ref.shape[1])]
        s = fdot(keys, qm_ref[head]).reshape(chunk // 8, 8, rows)
        s_ref[slot, j] = s
        return jnp.maximum(top, jnp.max(s, axis=0))

    def set_top(slot, top):
        m_ref[slot] = jnp.broadcast_to(jnp.max(top, axis=0, keepdims=True), top.shape)

    def values(head, j, slot, total, acc):
        e = jnp.exp2((s_ref[slot, j] - m_ref[slot][None]) * scale)
        vt = vt_ref[j, pl.ds(pl.multiple_of(head * head_dim, head_dim), head_dim), :]
        return total + jnp.sum(e, axis=0), acc + fdot(vt, e.reshape(chunk, rows).astype(jnp.bfloat16))

    def put_out(head, total, acc):
        out = acc * (1.0 / jnp.sum(total, axis=0, keepdims=True))
        ot_ref[pl.ds(pl.multiple_of(head * head_dim, head_dim), head_dim), :] = out.astype(jnp.bfloat16)

    low = jnp.full((8, rows), -jnp.inf, jnp.float32)
    none = jnp.zeros((8, rows), jnp.float32)
    zero = jnp.zeros((head_dim, rows), jnp.float32)

    def phase_body(phase, carry):
        clip = lax.rem(phase, n_clips)
        layer = phase // n_clips
        more = phase + 1 < phases
        ring.finish(phase)
        pl.when(more)(lambda: ring.begin(phase + 1))

        def project(r, carry):
            a = gath[phase, r].reshape(chunk, width)
            k_ref[r] = fdot(a, wqkv[layer, 1], NT).astype(jnp.bfloat16)
            vt_ref[r] = fdot(wqkv[layer, 2], a, NT).astype(jnp.bfloat16)
            return carry

        lax.fori_loop(0, n_chips, project, 0)
        qt = fdot(wqkv[layer, 0], gath[phase, 0, 0], NT).astype(jnp.bfloat16)
        for head in range(n_heads):
            at = (head % lane_heads) * head_dim
            qm_ref[head, at:at + head_dim, :] = qt[head * head_dim:(head + 1) * head_dim]

        top = low
        for j in range(n_chips):
            top = scores(0, j, 0, top)
        set_top(0, top)

        def head_body(head, carry):
            now = lax.rem(head, 2)
            turn = head - 2
            pl.when(more & (turn >= 0) & (lax.rem(turn, 2) == 0) & (turn // 2 < ring.arrivals))(
                lambda: ring.relay(phase + 1, turn // 2))
            top, total, acc = low, none, zero
            for j in range(n_chips):
                top = scores(head + 1, j, 1 - now, top)
                total, acc = values(head, j, now, total, acc)
            set_top(1 - now, top)
            put_out(head, total, acc)
            return carry

        lax.fori_loop(0, n_heads - 1, head_body, 0)
        total, acc = none, zero
        for j in range(n_chips):
            total, acc = values(n_heads - 1, j, (n_heads - 1) % 2, total, acc)
        put_out(n_heads - 1, total, acc)

        mid = (state[clip].astype(jnp.float32) + fdot(ot_ref[...], wproj[layer], TN)).astype(jnp.bfloat16)
        normed = layer_norm(mid)
        down = mid.astype(jnp.float32)
        for f in range(0, wup.shape[2], width):
            act = gelu(fdot(normed, wup[layer, :, f:f + width])).astype(jnp.bfloat16)
            down = down + fdot(act, wdown[layer, f:f + width, :])
        new = down.astype(jnp.bfloat16)
        state[clip] = new

        @pl.when(phase + n_clips < phases)
        def _():
            gath[phase + n_clips, 0, 0] = layer_norm(new)

        return carry

    lax.fori_loop(0, phases, phase_body, 0)


def run_decoder(n_chips, u, w_qkv, w_proj, w_up, w_down):
    n_clips, rows, width = u.shape
    n_layers, _, _, n_heads, head_dim = w_qkv.shape
    phases = n_layers * n_clips
    w_qkv = jnp.transpose(w_qkv, (0, 2, 3, 4, 1)).reshape(n_layers, 3, width, width)
    w_proj = w_proj.reshape(n_layers, width, width)
    mlp = w_up.shape[2]
    bf = jnp.bfloat16
    vmem, hbm = pl.BlockSpec(memory_space=pltpu.VMEM), pl.BlockSpec(memory_space=pl.ANY)
    keys = 2 * n_chips * rows
    return pl.pallas_call(
        functools.partial(decoder_kernel, n_chips, n_heads),
        out_shape=jax.ShapeDtypeStruct(u.shape, bf),
        in_specs=[vmem, hbm, hbm, hbm, hbm],
        out_specs=vmem,
        scratch_shapes=[
            pltpu.VMEM((phases, n_chips, 2, rows, width), bf),
            pltpu.VMEM((n_chips, 2 * rows, width), bf),
            pltpu.VMEM((n_chips, width, 2 * rows), bf),
            pltpu.VMEM((2, n_chips, rows // 4, 8, rows), jnp.float32),
            pltpu.VMEM((2, 8, rows), jnp.float32),
            pltpu.VMEM((n_heads, 256, rows), bf),
            pltpu.VMEM((width, rows), bf),
            pltpu.VMEM((n_layers, 3, width, width), bf),
            pltpu.VMEM((n_layers, width, width), bf),
            pltpu.VMEM((n_layers, width, mlp), bf),
            pltpu.VMEM((n_layers, mlp, width), bf),
            pltpu.SemaphoreType.DMA((phases, 3, n_chips, PIECES)),
            pltpu.SemaphoreType.DMA((phases, 3, n_chips, PIECES)),
            pltpu.SemaphoreType.DMA((4,)),
        ],
        compiler_params=pltpu.CompilerParams(collective_id=1, has_side_effects=True, vmem_limit_bytes=60 * 1024 * 1024),
        cost_estimate=pl.CostEstimate(flops=phases * n_heads * keys * rows * 2 * (256 + head_dim), bytes_accessed=16 * 1024 * 1024, transcendentals=phases * n_heads * keys * rows),
        name='decoder',
    )(u, w_qkv, w_proj, w_up, w_down)


def solution(mesh):
    group_size = mesh.shape['sp']
    to_next = [(src_dev, src_dev + 1) for src_dev in range(group_size - 1)]
    to_prev = [(src_dev + 1, src_dev) for src_dev in range(group_size - 1)]

    def local_program(patches, vis_mask, enc_pos, dec_pos, w_pe, b_pe, enc_qkv, enc_proj, enc_up, enc_down, w_ed, mask_token, dec_qkv, dec_proj, dec_up, dec_down, w_out):
        vis_shard = patches.shape[1] // KEEP_DIV
        half_rows = vis_shard // 2
        my_index = lax.axis_index('sp')
        vis_counts = lax.all_gather(jnp.sum(vis_mask, axis=1), 'sp')
        vis_before = jnp.sum(jnp.where(jnp.arange(group_size)[:, None] < my_index, vis_counts, 0), axis=0)
        local_rank = jnp.cumsum(vis_mask, axis=1) - vis_mask
        dest_row = vis_before[:, None] + local_rank - my_index * vis_shard + half_rows
        row_ids = jnp.arange(2 * vis_shard)
        select = ((dest_row[:, None, :] == row_ids[None, :, None]) & (vis_mask[:, None, :] == 1)).astype(jnp.bfloat16)
        moved_x = jnp.einsum('cqi,cip->cqp', select, patches, preferred_element_type=jnp.float32).astype(jnp.bfloat16)
        moved_pos = jnp.einsum('cqi,id->cqd', select, enc_pos, preferred_element_type=jnp.float32)
        occupied = jnp.sum(select, axis=2, dtype=jnp.float32)
        embedded = (jnp.einsum('cqp,pd->cqd', moved_x, w_pe, preferred_element_type=jnp.float32)
                    + occupied[:, :, None] * b_pe.astype(jnp.float32) + moved_pos).astype(jnp.bfloat16)
        from_prev = lax.ppermute(embedded[:, 3 * half_rows:], 'sp', to_next)
        from_next = lax.ppermute(embedded[:, :half_rows], 'sp', to_prev)
        hidden = embedded[:, half_rows:3 * half_rows] + jnp.concatenate([from_prev, from_next], axis=1)
        for layer_idx in range(enc_qkv.shape[0]):
            hidden = attn_mlp_block(hidden, enc_qkv[layer_idx], enc_proj[layer_idx], enc_up[layer_idx], enc_down[layer_idx])
        z_enc = jnp.einsum('cnd,de->cne', layer_norm(hidden), w_ed, preferred_element_type=jnp.float32).astype(jnp.bfloat16)
        z_prev = lax.ppermute(z_enc[:, half_rows:], 'sp', to_next)
        z_next = lax.ppermute(z_enc[:, :half_rows], 'sp', to_prev)
        z_rows = jnp.concatenate([z_prev, z_enc, z_next], axis=1)
        placed = jnp.einsum('cqi,cqe->cie', select, z_rows, preferred_element_type=jnp.float32)
        masked_part = (1 - vis_mask).astype(jnp.float32)[:, :, None] * mask_token.astype(jnp.float32)
        hidden = (placed + masked_part + dec_pos.astype(jnp.float32)).astype(jnp.bfloat16)
        hidden = run_decoder(group_size // 2, hidden, dec_qkv, dec_proj, dec_up, dec_down)
        return jnp.einsum('cne,ep->cnp', layer_norm(hidden), w_out, preferred_element_type=jnp.float32)

    row_spec = P('dp', 'sp', None)
    pos_spec = P(('dp', 'sp'), None)
    arg_specs = (row_spec, P('dp', 'sp'), pos_spec, pos_spec) + (P(),) * 13
    return jax.shard_map(local_program, mesh=mesh, in_specs=arg_specs, out_specs=row_spec, check_vma=False)
```

```python
import functools

import jax
import jax.numpy as jnp
from jax import lax
from jax.experimental import pallas as pl
from jax.experimental.pallas import tpu as pltpu
from jax.sharding import PartitionSpec as P

KEEP_DIV = 8
PIECES = 2
MESH = pl.DeviceIdType.MESH
LOG2E = 1.4426950408889634
NT = (((1,), (1,)), ((), ()))
TN = (((0,), (0,)), ((), ()))


def layer_norm(hidden):
    hid_f32 = hidden.astype(jnp.float32)
    centred = hid_f32 - jnp.mean(hid_f32, axis=-1, keepdims=True)
    row_var = jnp.mean(centred * centred, axis=-1, keepdims=True)
    return (centred * lax.rsqrt(row_var + 1e-6)).astype(jnp.bfloat16)


def gelu(x):
    return 0.5 * x * (1.0 + lax.erf(x * 0.7071067811865476))


def fdot(lhs, rhs, dims=(((1,), (0,)), ((), ()))):
    return lax.dot_general(lhs, rhs, dims, preferred_element_type=jnp.float32)


def attn_mlp_block(hidden, w_qkv, w_proj, w_up, w_down):
    proj_qkv = jnp.einsum('cnd,dshk->scnhk', layer_norm(hidden), w_qkv, preferred_element_type=jnp.float32).astype(jnp.bfloat16)
    kv_all = lax.all_gather(proj_qkv[1:], 'sp', axis=2, tiled=True)
    scores = jnp.einsum('cqhk,cshk->chqs', proj_qkv[0], kv_all[0], preferred_element_type=jnp.float32) * proj_qkv.shape[-1] ** -0.5
    attn_probs = jax.nn.softmax(scores, axis=-1).astype(jnp.bfloat16)
    attended = jnp.einsum('chqs,cshk->cqhk', attn_probs, kv_all[1], preferred_element_type=jnp.float32).astype(jnp.bfloat16)
    mid_state = (hidden + jnp.einsum('cqhk,hkd->cqd', attended, w_proj, preferred_element_type=jnp.float32)).astype(jnp.bfloat16)
    up_act = jax.nn.gelu(jnp.einsum('cnd,df->cnf', layer_norm(mid_state), w_up, preferred_element_type=jnp.float32), approximate=False).astype(jnp.bfloat16)
    return (mid_state + jnp.einsum('cnf,fd->cnd', up_act, w_down, preferred_element_type=jnp.float32)).astype(jnp.bfloat16)


class RingGather:
    def __init__(self, n_chips, piece_rows, buf, send, recv):
        self.n, self.rows, self.buf, self.send, self.recv = n_chips, piece_rows, buf, send, recv
        me = lax.axis_index('sp')
        size = 2 * n_chips
        self.right = lax.rem(me + 2, size)
        self.left = lax.rem(me + size - 2, size)
        self.mate = me + 1 - 2 * lax.rem(me, 2)
        self.arrivals = PIECES * (n_chips // 2) - 1

    def barrier(self):
        sem = pltpu.get_barrier_semaphore()
        for peer in (self.left, self.right, self.mate):
            pl.semaphore_signal(sem, inc=1, device_id={'sp': peer}, device_id_type=MESH)
        pl.semaphore_wait(sem, 3)

    def copy(self, phase, kind, step, piece):
        if kind == 2:
            src, dst, dst_core, peer = step, step, 1, self.mate
        elif kind == 0:
            src, dst, dst_core, peer = step, step + 1, 0, self.right
        else:
            src, dst, dst_core, peer = lax.rem(self.n - step, self.n), self.n - 1 - step, 0, self.left
        rows = pl.ds(pl.multiple_of(piece * self.rows, self.rows), self.rows)
        return pltpu.make_async_remote_copy(
            src_ref=self.buf.at[phase, src, 0, rows], dst_ref=self.buf.at[phase, dst, dst_core, rows],
            send_sem=self.send.at[phase, kind, step, piece], recv_sem=self.recv.at[phase, kind, step, piece],
            device_id={'sp': peer}, device_id_type=MESH)

    def begin(self, phase):
        for piece in range(PIECES):
            self.copy(phase, 0, 0, piece).start()
            self.copy(phase, 1, 0, PIECES - 1 - piece).start()
            self.copy(phase, 2, 0, piece).start()

    def relay(self, phase, k):
        step = k // PIECES
        p_right = lax.rem(k, PIECES)
        p_left = PIECES - 1 - p_right
        self.copy(phase, 0, step, p_right).wait_recv()
        pl.when(k < self.arrivals - PIECES)(lambda: self.copy(phase, 0, step + 1, p_right).start())
        self.copy(phase, 2, step + 1, p_right).start()
        self.copy(phase, 1, step, p_left).wait_recv()
        pl.when(k < self.arrivals - PIECES)(lambda: self.copy(phase, 1, step + 1, p_left).start())
        self.copy(phase, 2, self.n - 1 - step, p_left).start()

    def take(self, phase, slot):
        for piece in range(PIECES):
            self.copy(phase, 2, slot, piece).wait_recv()

    def drain(self, phases):
        def per_slot(i, carry):
            slot = lax.rem(i // PIECES, self.n)
            self.copy(i // (PIECES * self.n), 2, slot, lax.rem(i, PIECES)).wait_send()
            return carry

        def per_hop(i, carry):
            phase, k = i // self.arrivals, lax.rem(i, self.arrivals)
            self.copy(phase, 0, k // PIECES, lax.rem(k, PIECES)).wait_send()
            self.copy(phase, 1, k // PIECES, PIECES - 1 - lax.rem(k, PIECES)).wait_send()
            return carry

        lax.fori_loop(0, phases * PIECES * self.n, per_slot, 0)
        lax.fori_loop(0, phases * self.arrivals, per_hop, 0)


def decoder_kernel(n_chips, n_heads, u_ref, wqkv_hbm, wproj_hbm, wup_hbm, wdown_hbm, state,
                   gath, k_ref, vt_ref, s_even, s_odd, m_ref, qm_ref, ot_ref, wqkv, wproj, wup, wdown, send, recv, wsem):
    n_clips, rows, width = u_ref.shape
    n_layers = wproj.shape[0]
    phases = n_layers * n_clips
    head_dim = width // n_heads
    lane_heads = qm_ref.shape[1] // head_dim
    chunk = 2 * rows
    scale = head_dim ** -0.5 * LOG2E
    s_both = (s_even, s_odd)
    ring = RingGather(n_chips, rows // PIECES, gath, send, recv)

    weights = [pltpu.make_async_copy(src, dst, wsem.at[i]) for i, (src, dst) in enumerate(
        ((wqkv_hbm, wqkv), (wproj_hbm, wproj), (wup_hbm, wup), (wdown_hbm, wdown)))]
    for copy in weights:
        copy.start()
    for clip in range(n_clips):
        state[clip] = u_ref[clip]
        gath[clip, 0, 0] = layer_norm(u_ref[clip])
    qm_ref[...] = jnp.zeros_like(qm_ref)
    ring.barrier()
    ring.begin(0)
    for copy in weights:
        copy.wait()

    def scores(head, j, slot, top):
        group = head // lane_heads
        keys = k_ref[j, :, pl.ds(pl.multiple_of(group * qm_ref.shape[1], qm_ref.shape[1]), qm_ref.shape[1])]
        s = fdot(keys, qm_ref[head]).reshape(chunk // 8, 8, rows)
        s_both[slot][j] = s
        return jnp.maximum(top, jnp.max(s, axis=0))

    def set_top(slot, top):
        m_ref[slot] = jnp.broadcast_to(jnp.max(top, axis=0, keepdims=True), top.shape)

    def values(head, j, slot, total, acc):
        e = jnp.exp2((s_both[slot][j] - m_ref[slot][None]) * scale)
        vt = vt_ref[j, pl.ds(pl.multiple_of(head * head_dim, head_dim), head_dim), :]
        return total + jnp.sum(e, axis=0), acc + fdot(vt, e.reshape(chunk, rows).astype(jnp.bfloat16))

    def put_out(head, total, acc):
        out = acc * (1.0 / jnp.sum(total, axis=0, keepdims=True))
        ot_ref[pl.ds(pl.multiple_of(head * head_dim, head_dim), head_dim), :] = out.astype(jnp.bfloat16)

    low = jnp.full((8, rows), -jnp.inf, jnp.float32)
    none = jnp.zeros((8, rows), jnp.float32)
    zero = jnp.zeros((head_dim, rows), jnp.float32)

    def phase_body(phase, carry):
        clip = lax.rem(phase, n_clips)
        layer = phase // n_clips
        more = phase + 1 < phases
        first = phase == 0
        pl.when(more & (phase > 0))(lambda: ring.begin(phase + 1))

        def project(i, carry):
            odd = lax.rem(i, 2)
            r = jnp.where(odd == 1, (i + 1) // 2, lax.rem(n_chips - i // 2, n_chips))
            pl.when(first & (odd == 1))(lambda: ring.relay(phase, i - 1))
            pl.when(first & (odd == 1) & (i < ring.arrivals))(lambda: ring.relay(phase, i))
            pl.when(more & first & (i == ring.arrivals - 1))(lambda: ring.begin(phase + 1))
            ring.take(phase, r)
            a = gath[phase, r].reshape(chunk, width)
            k_ref[r] = fdot(a, wqkv[layer, 1], NT).astype(jnp.bfloat16)
            vt_ref[r] = fdot(wqkv[layer, 2], a, NT).astype(jnp.bfloat16)
            return carry

        lax.fori_loop(0, n_chips, project, 0)
        qt = fdot(wqkv[layer, 0], gath[phase, 0, 0], NT).astype(jnp.bfloat16)
        for head in range(n_heads):
            at = (head % lane_heads) * head_dim
            qm_ref[head, at:at + head_dim, :] = qt[head * head_dim:(head + 1) * head_dim]

        top = low
        for j in range(n_chips):
            top = scores(0, j, 0, top)
        set_top(0, top)

        def head_step(head, now, last=False):
            top, total, acc = low, none, zero
            for j in range(n_chips):
                if not last:
                    top = scores(head + 1, j, 1 - now, top)
                total, acc = values(head, j, now, total, acc)
            if not last:
                set_top(1 - now, top)
            put_out(head, total, acc)

        def head_pair(pair, carry):
            late = (pair > 2).astype(jnp.int32) + (pair > 5).astype(jnp.int32)
            pl.when(more & (pair != 2) & (pair != 5))(lambda: ring.relay(phase + 1, pair - late))
            head_step(2 * pair, 0)
            head_step(2 * pair + 1, 1)
            return carry

        lax.fori_loop(0, n_heads // 2 - 1, head_pair, 0)
        pl.when(more)(lambda: ring.relay(phase + 1, ring.arrivals - 2))
        head_step(n_heads - 2, 0)
        head_step(n_heads - 1, 1, last=True)

        mid = (state[clip].astype(jnp.float32) + fdot(ot_ref[...], wproj[layer], TN)).astype(jnp.bfloat16)
        normed = layer_norm(mid)
        down = mid.astype(jnp.float32)
        for f in range(0, wup.shape[2], width):
            act = gelu(fdot(normed, wup[layer, :, f:f + width])).astype(jnp.bfloat16)
            down = down + fdot(act, wdown[layer, f:f + width, :])
        new = down.astype(jnp.bfloat16)
        state[clip] = new

        @pl.when(phase + n_clips < phases)
        def _():
            gath[phase + n_clips, 0, 0] = layer_norm(new)

        pl.when(more)(lambda: ring.relay(phase + 1, ring.arrivals - 1))
        return carry

    lax.fori_loop(0, phases, phase_body, 0)
    ring.drain(phases)


def run_decoder(n_chips, u, w_qkv, w_proj, w_up, w_down):
    n_clips, rows, width = u.shape
    n_layers, _, _, n_heads, head_dim = w_qkv.shape
    phases = n_layers * n_clips
    w_qkv = jnp.transpose(w_qkv, (0, 2, 3, 4, 1)).reshape(n_layers, 3, width, width)
    w_proj = w_proj.reshape(n_layers, width, width)
    mlp = w_up.shape[2]
    bf = jnp.bfloat16
    vmem, hbm = pl.BlockSpec(memory_space=pltpu.VMEM), pl.BlockSpec(memory_space=pl.ANY)
    keys = 2 * n_chips * rows
    return pl.pallas_call(
        functools.partial(decoder_kernel, n_chips, n_heads),
        out_shape=jax.ShapeDtypeStruct(u.shape, bf),
        in_specs=[vmem, hbm, hbm, hbm, hbm],
        out_specs=vmem,
        scratch_shapes=[
            pltpu.VMEM((phases, n_chips, 2, rows, width), bf),
            pltpu.VMEM((n_chips, 2 * rows, width), bf),
            pltpu.VMEM((n_chips, width, 2 * rows), bf),
            pltpu.VMEM((n_chips, rows // 4, 8, rows), jnp.float32),
            pltpu.VMEM((n_chips, rows // 4, 8, rows), jnp.float32),
            pltpu.VMEM((2, 8, rows), jnp.float32),
            pltpu.VMEM((n_heads, 256, rows), bf),
            pltpu.VMEM((width, rows), bf),
            pltpu.VMEM((n_layers, 3, width, width), bf),
            pltpu.VMEM((n_layers, width, width), bf),
            pltpu.VMEM((n_layers, width, mlp), bf),
            pltpu.VMEM((n_layers, mlp, width), bf),
            pltpu.SemaphoreType.DMA((phases, 3, n_chips, PIECES)),
            pltpu.SemaphoreType.DMA((phases, 3, n_chips, PIECES)),
            pltpu.SemaphoreType.DMA((4,)),
        ],
        compiler_params=pltpu.CompilerParams(collective_id=1, has_side_effects=True, vmem_limit_bytes=60 * 1024 * 1024),
        cost_estimate=pl.CostEstimate(flops=phases * n_heads * keys * rows * 2 * (256 + head_dim), bytes_accessed=16 * 1024 * 1024, transcendentals=phases * n_heads * keys * rows),
        name='decoder',
    )(u, w_qkv, w_proj, w_up, w_down)


def solution(mesh):
    group_size = mesh.shape['sp']
    to_next = [(src_dev, src_dev + 1) for src_dev in range(group_size - 1)]
    to_prev = [(src_dev + 1, src_dev) for src_dev in range(group_size - 1)]

    def local_program(patches, vis_mask, enc_pos, dec_pos, w_pe, b_pe, enc_qkv, enc_proj, enc_up, enc_down, w_ed, mask_token, dec_qkv, dec_proj, dec_up, dec_down, w_out):
        vis_shard = patches.shape[1] // KEEP_DIV
        half_rows = vis_shard // 2
        my_index = lax.axis_index('sp')
        vis_counts = lax.all_gather(jnp.sum(vis_mask, axis=1), 'sp')
        vis_before = jnp.sum(jnp.where(jnp.arange(group_size)[:, None] < my_index, vis_counts, 0), axis=0)
        local_rank = jnp.cumsum(vis_mask, axis=1) - vis_mask
        dest_row = vis_before[:, None] + local_rank - my_index * vis_shard + half_rows
        row_ids = jnp.arange(2 * vis_shard)
        select = ((dest_row[:, None, :] == row_ids[None, :, None]) & (vis_mask[:, None, :] == 1)).astype(jnp.bfloat16)
        moved_x = jnp.einsum('cqi,cip->cqp', select, patches, preferred_element_type=jnp.float32).astype(jnp.bfloat16)
        moved_pos = jnp.einsum('cqi,id->cqd', select, enc_pos, preferred_element_type=jnp.float32)
        occupied = jnp.sum(select, axis=2, dtype=jnp.float32)
        embedded = (jnp.einsum('cqp,pd->cqd', moved_x, w_pe, preferred_element_type=jnp.float32)
                    + occupied[:, :, None] * b_pe.astype(jnp.float32) + moved_pos).astype(jnp.bfloat16)
        from_prev = lax.ppermute(embedded[:, 3 * half_rows:], 'sp', to_next)
        from_next = lax.ppermute(embedded[:, :half_rows], 'sp', to_prev)
        hidden = embedded[:, half_rows:3 * half_rows] + jnp.concatenate([from_prev, from_next], axis=1)
        for layer_idx in range(enc_qkv.shape[0]):
            hidden = attn_mlp_block(hidden, enc_qkv[layer_idx], enc_proj[layer_idx], enc_up[layer_idx], enc_down[layer_idx])
        z_enc = jnp.einsum('cnd,de->cne', layer_norm(hidden), w_ed, preferred_element_type=jnp.float32).astype(jnp.bfloat16)
        z_prev = lax.ppermute(z_enc[:, half_rows:], 'sp', to_next)
        z_next = lax.ppermute(z_enc[:, :half_rows], 'sp', to_prev)
        z_rows = jnp.concatenate([z_prev, z_enc, z_next], axis=1)
        placed = jnp.einsum('cqi,cqe->cie', select, z_rows, preferred_element_type=jnp.float32)
        masked_part = (1 - vis_mask).astype(jnp.float32)[:, :, None] * mask_token.astype(jnp.float32)
        hidden = (placed + masked_part + dec_pos.astype(jnp.float32)).astype(jnp.bfloat16)
        hidden = run_decoder(group_size // 2, hidden, dec_qkv, dec_proj, dec_up, dec_down)
        return jnp.einsum('cne,ep->cnp', layer_norm(hidden), w_out, preferred_element_type=jnp.float32)

    row_spec = P('dp', 'sp', None)
    pos_spec = P(('dp', 'sp'), None)
    arg_specs = (row_spec, P('dp', 'sp'), pos_spec, pos_spec) + (P(),) * 13
    return jax.shard_map(local_program, mesh=mesh, in_specs=arg_specs, out_specs=row_spec, check_vma=False)
```

```python
import functools

import jax
import jax.numpy as jnp
from jax import lax
from jax.experimental import pallas as pl
from jax.experimental.pallas import tpu as pltpu
from jax.sharding import PartitionSpec as P

KEEP_DIV = 8
PIECES = 2
MESH = pl.DeviceIdType.MESH
LOG2E = 1.4426950408889634
NT = (((1,), (1,)), ((), ()))
TN = (((0,), (0,)), ((), ()))


def layer_norm(hidden):
    hid_f32 = hidden.astype(jnp.float32)
    centred = hid_f32 - jnp.mean(hid_f32, axis=-1, keepdims=True)
    row_var = jnp.mean(centred * centred, axis=-1, keepdims=True)
    return (centred * lax.rsqrt(row_var + 1e-6)).astype(jnp.bfloat16)


def gelu(x):
    return 0.5 * x * (1.0 + lax.erf(x * 0.7071067811865476))


def fdot(lhs, rhs, dims=(((1,), (0,)), ((), ()))):
    return lax.dot_general(lhs, rhs, dims, preferred_element_type=jnp.float32)


class RingGather:
    def __init__(self, n_chips, piece_rows, buf, send, recv):
        self.n, self.rows, self.buf, self.send, self.recv = n_chips, piece_rows, buf, send, recv
        me = lax.axis_index('sp')
        size = 2 * n_chips
        self.right = lax.rem(me + 2, size)
        self.left = lax.rem(me + size - 2, size)
        self.mate = me + 1 - 2 * lax.rem(me, 2)
        self.arrivals = PIECES * (n_chips // 2) - 1

    def barrier(self):
        sem = pltpu.get_barrier_semaphore()
        for peer in (self.left, self.right, self.mate):
            pl.semaphore_signal(sem, inc=1, device_id={'sp': peer}, device_id_type=MESH)
        pl.semaphore_wait(sem, 3)

    def copy(self, phase, kind, step, piece):
        if kind == 2:
            src, dst, dst_core, peer = step, step, 1, self.mate
        elif kind == 0:
            src, dst, dst_core, peer = step, step + 1, 0, self.right
        else:
            src, dst, dst_core, peer = lax.rem(self.n - step, self.n), self.n - 1 - step, 0, self.left
        rows = pl.ds(pl.multiple_of(piece * self.rows, self.rows), self.rows)
        return pltpu.make_async_remote_copy(
            src_ref=self.buf.at[phase, src, 0, rows], dst_ref=self.buf.at[phase, dst, dst_core, rows],
            send_sem=self.send.at[phase, kind, step, piece], recv_sem=self.recv.at[phase, kind, step, piece],
            device_id={'sp': peer}, device_id_type=MESH)

    def begin(self, phase):
        for piece in range(PIECES):
            self.copy(phase, 0, 0, piece).start()
            self.copy(phase, 1, 0, PIECES - 1 - piece).start()
            self.copy(phase, 2, 0, piece).start()

    def relay(self, phase, k):
        step = k // PIECES
        p_right = lax.rem(k, PIECES)
        p_left = PIECES - 1 - p_right
        self.copy(phase, 0, step, p_right).wait_recv()
        pl.when(k < self.arrivals - PIECES)(lambda: self.copy(phase, 0, step + 1, p_right).start())
        self.copy(phase, 2, step + 1, p_right).start()
        self.copy(phase, 1, step, p_left).wait_recv()
        pl.when(k < self.arrivals - PIECES)(lambda: self.copy(phase, 1, step + 1, p_left).start())
        self.copy(phase, 2, self.n - 1 - step, p_left).start()

    def take(self, phase, slot):
        for piece in range(PIECES):
            self.copy(phase, 2, slot, piece).wait_recv()

    def drain(self, phases):
        def per_slot(i, carry):
            slot = lax.rem(i // PIECES, self.n)
            self.copy(i // (PIECES * self.n), 2, slot, lax.rem(i, PIECES)).wait_send()
            return carry

        def per_hop(i, carry):
            phase, k = i // self.arrivals, lax.rem(i, self.arrivals)
            self.copy(phase, 0, k // PIECES, lax.rem(k, PIECES)).wait_send()
            self.copy(phase, 1, k // PIECES, PIECES - 1 - lax.rem(k, PIECES)).wait_send()
            return carry

        lax.fori_loop(0, phases * PIECES * self.n, per_slot, 0)
        lax.fori_loop(0, phases * self.arrivals, per_hop, 0)


def decoder_kernel(n_chips, n_heads, u_ref, wqkv_hbm, wproj_hbm, wup_hbm, wdown_hbm, state,
                   gath, k_ref, vt_ref, s_even, s_odd, m_ref, qm_ref, ot_ref, wqkv, wproj, wup, wdown, send, recv, wsem):
    n_clips, rows, width = u_ref.shape
    n_layers = wproj.shape[0]
    phases = n_layers * n_clips
    head_dim = width // n_heads
    lane_heads = qm_ref.shape[1] // head_dim
    chunk = 2 * rows
    scale = head_dim ** -0.5 * LOG2E
    s_both = (s_even, s_odd)
    ring = RingGather(n_chips, rows // PIECES, gath, send, recv)

    weights = [pltpu.make_async_copy(src, dst, wsem.at[i]) for i, (src, dst) in enumerate(
        ((wqkv_hbm, wqkv), (wproj_hbm, wproj), (wup_hbm, wup), (wdown_hbm, wdown)))]
    for copy in weights:
        copy.start()
    for clip in range(n_clips):
        state[clip] = u_ref[clip]
        gath[clip, 0, 0] = layer_norm(u_ref[clip])
    qm_ref[...] = jnp.zeros_like(qm_ref)
    ring.barrier()
    ring.begin(0)
    for copy in weights:
        copy.wait()

    def scores(head, j, slot, top):
        group = head // lane_heads
        keys = k_ref[j, :, pl.ds(pl.multiple_of(group * qm_ref.shape[1], qm_ref.shape[1]), qm_ref.shape[1])]
        s = fdot(keys, qm_ref[head]).reshape(chunk // 8, 8, rows)
        s_both[slot][j] = s
        return jnp.maximum(top, jnp.max(s, axis=0))

    def set_top(slot, top):
        m_ref[slot] = jnp.broadcast_to(jnp.max(top, axis=0, keepdims=True), top.shape)

    def values(head, j, slot, total, acc):
        e = jnp.exp2((s_both[slot][j] - m_ref[slot][None]) * scale)
        vt = vt_ref[j, pl.ds(pl.multiple_of(head * head_dim, head_dim), head_dim), :]
        return total + jnp.sum(e, axis=0), acc + fdot(vt, e.reshape(chunk, rows).astype(jnp.bfloat16))

    def put_out(head, total, acc):
        out = acc * (1.0 / jnp.sum(total, axis=0, keepdims=True))
        ot_ref[pl.ds(pl.multiple_of(head * head_dim, head_dim), head_dim), :] = out.astype(jnp.bfloat16)

    low = jnp.full((8, rows), -jnp.inf, jnp.float32)
    none = jnp.zeros((8, rows), jnp.float32)
    zero = jnp.zeros((head_dim, rows), jnp.float32)

    def phase_body(phase, carry):
        clip = lax.rem(phase, n_clips)
        layer = phase // n_clips
        more = phase + 1 < phases
        first = phase == 0
        pl.when(more & (phase > 0))(lambda: ring.begin(phase + 1))

        def project(i, carry):
            odd = lax.rem(i, 2)
            r = jnp.where(odd == 1, (i + 1) // 2, lax.rem(n_chips - i // 2, n_chips))
            pl.when(first & (odd == 1))(lambda: ring.relay(phase, i - 1))
            pl.when(first & (odd == 1) & (i < ring.arrivals))(lambda: ring.relay(phase, i))
            pl.when(more & first & (i == ring.arrivals - 1))(lambda: ring.begin(phase + 1))
            ring.take(phase, r)
            a = gath[phase, r].reshape(chunk, width)
            k_ref[r] = fdot(a, wqkv[layer, 1], NT).astype(jnp.bfloat16)
            vt_ref[r] = fdot(wqkv[layer, 2], a, NT).astype(jnp.bfloat16)
            return carry

        lax.fori_loop(0, n_chips, project, 0)
        qt = fdot(wqkv[layer, 0], gath[phase, 0, 0], NT).astype(jnp.bfloat16)
        for head in range(n_heads):
            at = (head % lane_heads) * head_dim
            qm_ref[head, at:at + head_dim, :] = qt[head * head_dim:(head + 1) * head_dim]

        top = low
        for j in range(n_chips):
            top = scores(0, j, 0, top)
        set_top(0, top)

        def head_step(head, now, last=False):
            top, total, acc = low, none, zero
            for j in range(n_chips):
                if not last:
                    top = scores(head + 1, j, 1 - now, top)
                total, acc = values(head, j, now, total, acc)
            if not last:
                set_top(1 - now, top)
            put_out(head, total, acc)

        def head_pair(pair, carry):
            late = (pair > 2).astype(jnp.int32) + (pair > 5).astype(jnp.int32)
            pl.when(more & (pair != 2) & (pair != 5))(lambda: ring.relay(phase + 1, pair - late))
            head_step(2 * pair, 0)
            head_step(2 * pair + 1, 1)
            return carry

        lax.fori_loop(0, n_heads // 2 - 1, head_pair, 0)
        pl.when(more)(lambda: ring.relay(phase + 1, ring.arrivals - 2))
        head_step(n_heads - 2, 0)
        head_step(n_heads - 1, 1, last=True)

        mid = (state[clip].astype(jnp.float32) + fdot(ot_ref[...], wproj[layer], TN)).astype(jnp.bfloat16)
        normed = layer_norm(mid)
        down = mid.astype(jnp.float32)
        for f in range(0, wup.shape[2], width):
            act = gelu(fdot(normed, wup[layer, :, f:f + width])).astype(jnp.bfloat16)
            down = down + fdot(act, wdown[layer, f:f + width, :])
        new = down.astype(jnp.bfloat16)
        state[clip] = new

        @pl.when(phase + n_clips < phases)
        def _():
            gath[phase + n_clips, 0, 0] = layer_norm(new)

        pl.when(more)(lambda: ring.relay(phase + 1, ring.arrivals - 1))
        return carry

    lax.fori_loop(0, phases, phase_body, 0)
    ring.drain(phases)


def run_decoder(n_chips, u, w_qkv, w_proj, w_up, w_down):
    n_clips, rows, width = u.shape
    n_layers, _, _, n_heads, head_dim = w_qkv.shape
    phases = n_layers * n_clips
    w_qkv = jnp.transpose(w_qkv, (0, 2, 3, 4, 1)).reshape(n_layers, 3, width, width)
    w_proj = w_proj.reshape(n_layers, width, width)
    mlp = w_up.shape[2]
    bf = jnp.bfloat16
    vmem, hbm = pl.BlockSpec(memory_space=pltpu.VMEM), pl.BlockSpec(memory_space=pl.ANY)
    keys = 2 * n_chips * rows
    return pl.pallas_call(
        functools.partial(decoder_kernel, n_chips, n_heads),
        out_shape=jax.ShapeDtypeStruct(u.shape, bf),
        in_specs=[vmem, hbm, hbm, hbm, hbm],
        out_specs=vmem,
        scratch_shapes=[
            pltpu.VMEM((phases, n_chips, 2, rows, width), bf),
            pltpu.VMEM((n_chips, 2 * rows, width), bf),
            pltpu.VMEM((n_chips, width, 2 * rows), bf),
            pltpu.VMEM((n_chips, rows // 4, 8, rows), jnp.float32),
            pltpu.VMEM((n_chips, rows // 4, 8, rows), jnp.float32),
            pltpu.VMEM((2, 8, rows), jnp.float32),
            pltpu.VMEM((n_heads, 256, rows), bf),
            pltpu.VMEM((width, rows), bf),
            pltpu.VMEM((n_layers, 3, width, width), bf),
            pltpu.VMEM((n_layers, width, width), bf),
            pltpu.VMEM((n_layers, width, mlp), bf),
            pltpu.VMEM((n_layers, mlp, width), bf),
            pltpu.SemaphoreType.DMA((phases, 3, n_chips, PIECES)),
            pltpu.SemaphoreType.DMA((phases, 3, n_chips, PIECES)),
            pltpu.SemaphoreType.DMA((4,)),
        ],
        compiler_params=pltpu.CompilerParams(collective_id=1, has_side_effects=True, vmem_limit_bytes=60 * 1024 * 1024),
        cost_estimate=pl.CostEstimate(flops=phases * n_heads * keys * rows * 2 * (256 + head_dim), bytes_accessed=16 * 1024 * 1024, transcendentals=phases * n_heads * keys * rows),
        name='decoder',
    )(u, w_qkv, w_proj, w_up, w_down)


def encoder_kernel(n_chips, n_heads, patches_hbm, mask_ref, epos_hbm, dpos_hbm, wpe_hbm, bias_ref, wqkv_hbm, wproj_hbm,
                   wup_hbm, wdown_hbm, wed_hbm, token_ref, u_ref,
                   patches, epos, dpos, wpe, wqkv, wproj, wup, wdown, wed,
                   gath, kvt, q_ref, o_ref, hid, mx_ref, sel_ref, shift_ref, emb_ref, place_ref, edge_ref, z_ref, count_ref,
                   send, recv, csend, crecv, esend, erecv, fsem, wsem):
    n_clips, tokens, _ = u_ref.shape
    n_layers, width = wproj.shape[0], wproj.shape[1]
    size = 2 * n_chips
    keep = hid.shape[0] // n_clips
    half = keep // 2
    slots = 2 * keep
    head_dim = width // n_heads
    lanes = 256
    pack = lanes // head_dim
    scale = head_dim ** -0.5 * LOG2E
    bf, f32 = jnp.bfloat16, jnp.float32
    ring = RingGather(n_chips, keep, gath, send, recv)
    me = lax.axis_index('sp')

    fetch = [pltpu.make_async_copy(src, dst, fsem.at[i]) for i, (src, dst) in enumerate(
        ((patches_hbm, patches), (wpe_hbm, wpe), (epos_hbm, epos), (dpos_hbm, dpos), (wed_hbm, wed)))]
    for copy in fetch:
        copy.start()

    def layer_copy(layer, i):
        src = (wqkv_hbm, wproj_hbm, wup_hbm, wdown_hbm)[i].at[layer]
        dst = (wqkv.at[layer], wproj.at[layer], wup, wdown)[i]
        return pltpu.make_async_copy(src, dst, wsem.at[layer, i])

    sem = pltpu.get_barrier_semaphore()

    def greet(t, carry):
        pl.semaphore_signal(sem, inc=1, device_id={'sp': lax.rem(me + t, size)}, device_id_type=MESH)
        return carry

    lax.fori_loop(1, size, greet, 0)

    row_id = lax.broadcasted_iota(jnp.int32, (slots, tokens), 0).astype(f32)
    earlier = (lax.broadcasted_iota(jnp.int32, (tokens, tokens), 0)
               < lax.broadcasted_iota(jnp.int32, (tokens, tokens), 1)).astype(f32).astype(bf)
    masks = [jnp.broadcast_to(mask_ref[c:c + 1, :].astype(f32), (8, tokens)) for c in range(n_clips)]
    line = lax.broadcasted_iota(jnp.int32, (8, 128), 0)
    mine = jnp.zeros((8, 128), f32)
    occupied = []
    for c in range(n_clips):
        mine = jnp.where(line == c, jnp.sum(masks[c], axis=1, keepdims=True), mine)
        rank = fdot(masks[c].astype(bf), earlier)
        sel = jnp.where((row_id == rank[0:1]) & (masks[c][0:1] > 0.5), 1.0, 0.0)
        occupied.append(jnp.sum(sel, axis=1, keepdims=True))
        sel_ref[c] = sel.astype(bf)
    count_ref[me] = mine
    pl.semaphore_wait(sem, size - 1)

    def count_copy(t):
        return pltpu.make_async_remote_copy(
            src_ref=count_ref.at[me], dst_ref=count_ref.at[me], send_sem=csend.at[t], recv_sem=crecv.at[t],
            device_id={'sp': lax.rem(me + t, size)}, device_id_type=MESH)

    def count_from(t):
        src = lax.rem(me + size - t, size)
        return pltpu.make_async_remote_copy(
            src_ref=count_ref.at[src], dst_ref=count_ref.at[src], send_sem=csend.at[t], recv_sem=crecv.at[t],
            device_id={'sp': lax.rem(me + t, size)}, device_id_type=MESH)

    lax.fori_loop(1, size, lambda t, carry: (count_copy(t).start(), carry)[1], 0)
    for copy in fetch[:3]:
        copy.wait()
    for i in range(4):
        layer_copy(0, i).start()
    for layer in range(1, n_layers):
        for i in range(2):
            layer_copy(layer, i).start()

    for c in range(n_clips):
        mx_ref[c * slots:(c + 1) * slots] = fdot(sel_ref[c], patches[c]).astype(bf)
    embedded = fdot(mx_ref[...], wpe[...])
    bias = bias_ref[...].astype(f32)
    for c in range(n_clips):
        emb_ref[c] = (embedded[c * slots:(c + 1) * slots] + occupied[c] * bias + fdot(sel_ref[c], epos[...])).astype(bf)

    lax.fori_loop(1, size, lambda t, carry: (count_from(t).wait_recv(), carry)[1], 0)
    source = lax.broadcasted_iota(jnp.int32, (size, 8, 128), 0)
    offset = (half - me * keep).astype(f32) + jnp.sum(jnp.where(source < me, count_ref[...], 0.0), axis=0)
    apart = (lax.broadcasted_iota(jnp.int32, (slots, slots), 0) - lax.broadcasted_iota(jnp.int32, (slots, slots), 1)).astype(f32)
    for c in range(n_clips):
        shift_ref[c] = jnp.where(apart == offset[c:c + 1, :slots], 1.0, 0.0).astype(bf)
        place_ref[c] = fdot(shift_ref[c], emb_ref[c]).astype(bf)

    after, before = lax.rem(me + 1, size), lax.rem(me + size - 1, size)

    def edge_copy(i, src, dst, peer):
        return pltpu.make_async_remote_copy(src_ref=src, dst_ref=dst, send_sem=esend.at[i], recv_sem=erecv.at[i],
                                            device_id={'sp': peer}, device_id_type=MESH)

    edges = [edge_copy(0, place_ref.at[:, pl.ds(slots - half, half)], edge_ref.at[0], after),
             edge_copy(1, place_ref.at[:, pl.ds(0, half)], edge_ref.at[1], before)]
    for copy in edges:
        copy.start()
    for copy in edges:
        copy.wait_recv()
    for c in range(n_clips):
        for i in range(2):
            hid[c * keep + i * half:c * keep + (i + 1) * half] = (
                place_ref[c, half + i * half:half + (i + 1) * half].astype(f32) + edge_ref[i, c].astype(f32)).astype(bf)
    gath[0, 0, 0] = layer_norm(hid[...])

    block = (lax.broadcasted_iota(jnp.int32, (pack * keep, lanes), 0) // keep
             == lax.broadcasted_iota(jnp.int32, (pack * keep, lanes), 1) // head_dim).astype(f32)
    block_bf = block.astype(bf)
    order = [0]
    for i in range(1, n_chips // 2):
        order += [i, n_chips - i]
    order.append(n_chips // 2)
    n_parts = 2
    part = n_chips // n_parts
    part_keys = part * 2 * keep

    def layer_body(layer, carry):
        ring.begin(layer)
        layer_copy(layer, 0).wait()
        q_ref[...] = fdot(gath[layer, 0, 0], wqkv[layer, :width], NT).astype(bf)
        for i in range(n_parts):
            picked = order[i * part:(i + 1) * part]
            ready = ring.arrivals if i == n_parts - 1 else PIECES * (n_chips // 4)
            done = 0 if i == 0 else PIECES * (n_chips // 4)
            lax.fori_loop(done, ready, lambda k, carry: (ring.relay(layer, k), carry)[1], 0)
            for slot in picked:
                ring.take(layer, slot)
            for c in range(n_clips):
                a = jnp.concatenate([gath[layer, slot, :, c * keep:(c + 1) * keep].reshape(2 * keep, width) for slot in picked], axis=0)
                kvt[c, :, i * part_keys:(i + 1) * part_keys] = fdot(wqkv[layer, width:], a, NT).astype(bf)

        for c in range(n_clips):
            for g in range(width // lanes):
                at = slice(g * lanes, (g + 1) * lanes)
                q = q_ref[c * keep:(c + 1) * keep, at]
                s = fdot(jnp.concatenate([q] * pack, axis=0) * block_bf, kvt[c, at, :])
                e = jnp.exp2((s - jnp.max(s, axis=1, keepdims=True)) * scale)
                p = (e * (1.0 / jnp.sum(e, axis=1, keepdims=True))).astype(bf)
                o = fdot(p, kvt[c, width + g * lanes:width + (g + 1) * lanes, :], NT) * block
                total = o[:keep]
                for h in range(1, pack):
                    total = total + o[h * keep:(h + 1) * keep]
                o_ref[c * keep:(c + 1) * keep, at] = total.astype(bf)

        layer_copy(layer, 1).wait()
        mid = (hid[...].astype(f32) + fdot(o_ref[...], wproj[layer])).astype(bf)
        normed = layer_norm(mid)
        down = mid.astype(f32)
        layer_copy(layer, 2).wait()
        layer_copy(layer, 3).wait()
        for f in range(0, wup.shape[1], width):
            act = gelu(fdot(normed, wup[:, f:f + width])).astype(bf)
            down = down + fdot(act, wdown[f:f + width, :])
        new = down.astype(bf)
        hid[...] = new

        @pl.when(layer + 1 < n_layers)
        def _():
            for i in (2, 3):
                layer_copy(layer + 1, i).start()
            gath[layer + 1, 0, 0] = layer_norm(new)

        return carry

    lax.fori_loop(0, n_layers, layer_body, 0)

    for copy in fetch[3:]:
        copy.wait()
    z = fdot(layer_norm(hid[...]), wed[...]).astype(bf)
    for c in range(n_clips):
        z_ref[c, half:half + keep] = z[c * keep:(c + 1) * keep]
    z_edges = [edge_copy(2, z_ref.at[:, pl.ds(keep, half)], z_ref.at[:, pl.ds(0, half)], after),
               edge_copy(3, z_ref.at[:, pl.ds(half, half)], z_ref.at[:, pl.ds(half + keep, half)], before)]
    for copy in z_edges:
        copy.start()
    first_line = lax.broadcasted_iota(jnp.int32, (8, tokens), 0) == 0
    token = jnp.broadcast_to(token_ref[...].astype(f32), (8, token_ref.shape[1])).astype(bf)
    hidden_part = [fdot(jnp.where(first_line, 1.0 - m, 0.0).astype(bf), token, TN) for m in masks]
    for copy in z_edges:
        copy.wait_recv()
    for c in range(n_clips):
        own = fdot(shift_ref[c], z_ref[c], TN).astype(bf)
        u_ref[c] = (fdot(sel_ref[c], own, TN) + hidden_part[c] + dpos[...].astype(f32)).astype(bf)

    lax.fori_loop(1, size, lambda t, carry: (count_copy(t).wait_send(), carry)[1], 0)
    for copy in edges + z_edges:
        copy.wait_send()
    ring.drain(n_layers)


def run_encoder(n_chips, patches, mask, enc_pos, dec_pos, w_pe, b_pe, w_qkv, w_proj, w_up, w_down, w_ed, token):
    n_clips, tokens, patch = patches.shape
    n_layers, width, _, n_heads, head_dim = w_qkv.shape
    mlp, out_width = w_up.shape[2], w_ed.shape[1]
    keep = tokens // KEEP_DIV
    rows, slots = n_clips * keep, 2 * keep
    bf, f32 = jnp.bfloat16, jnp.float32
    w_qkv = jnp.transpose(w_qkv, (0, 2, 3, 4, 1)).reshape(n_layers, 3 * width, width)
    w_proj = w_proj.reshape(n_layers, width, width)
    vmem, hbm = pl.BlockSpec(memory_space=pltpu.VMEM), pl.BlockSpec(memory_space=pl.ANY)
    dma = pltpu.SemaphoreType.DMA
    keys = 2 * n_chips * keep
    flops = 2 * n_layers * rows * width * (4 * width + 2 * mlp) + 4 * n_layers * keys * n_clips * width * width
    return pl.pallas_call(
        functools.partial(encoder_kernel, n_chips, n_heads),
        out_shape=jax.ShapeDtypeStruct((n_clips, tokens, out_width), bf),
        in_specs=[hbm, vmem, hbm, hbm, hbm, vmem, hbm, hbm, hbm, hbm, hbm, vmem],
        out_specs=vmem,
        scratch_shapes=[
            pltpu.VMEM(patches.shape, bf), pltpu.VMEM(enc_pos.shape, bf), pltpu.VMEM(dec_pos.shape, bf),
            pltpu.VMEM(w_pe.shape, bf), pltpu.VMEM(w_qkv.shape, bf), pltpu.VMEM(w_proj.shape, bf),
            pltpu.VMEM(w_up.shape[1:], bf), pltpu.VMEM(w_down.shape[1:], bf), pltpu.VMEM(w_ed.shape, bf),
            pltpu.VMEM((n_layers, n_chips, 2, rows, width), bf),
            pltpu.VMEM((n_clips, 2 * width, keys), bf),
            pltpu.VMEM((rows, width), bf), pltpu.VMEM((rows, width), bf), pltpu.VMEM((rows, width), bf),
            pltpu.VMEM((n_clips * slots, patch), bf),
            pltpu.VMEM((n_clips, slots, tokens), bf), pltpu.VMEM((n_clips, slots, slots), bf),
            pltpu.VMEM((n_clips, slots, width), bf), pltpu.VMEM((n_clips, slots, width), bf),
            pltpu.VMEM((2, n_clips, keep // 2, width), bf), pltpu.VMEM((n_clips, slots, out_width), bf),
            pltpu.VMEM((2 * n_chips, 8, 128), f32),
            dma((n_layers, 3, n_chips, PIECES)), dma((n_layers, 3, n_chips, PIECES)),
            dma((2 * n_chips,)), dma((2 * n_chips,)), dma((4,)), dma((4,)), dma((5,)), dma((n_layers, 4)),
        ],
        compiler_params=pltpu.CompilerParams(collective_id=2, has_side_effects=True, vmem_limit_bytes=60 * 1024 * 1024),
        cost_estimate=pl.CostEstimate(flops=flops, bytes_accessed=56 * 1024 * 1024, transcendentals=0),
        name='encoder',
    )(patches, mask, enc_pos, dec_pos, w_pe, b_pe.reshape(1, -1), w_qkv, w_proj, w_up, w_down, w_ed, token.reshape(1, -1))


def solution(mesh):
    n_chips = mesh.shape['sp'] // 2

    def local_program(patches, vis_mask, enc_pos, dec_pos, w_pe, b_pe, enc_qkv, enc_proj, enc_up, enc_down, w_ed, mask_token, dec_qkv, dec_proj, dec_up, dec_down, w_out):
        hidden = run_encoder(n_chips, patches, vis_mask, enc_pos, dec_pos, w_pe, b_pe, enc_qkv, enc_proj, enc_up, enc_down, w_ed, mask_token)
        hidden = run_decoder(n_chips, hidden, dec_qkv, dec_proj, dec_up, dec_down)
        return jnp.einsum('cne,ep->cnp', layer_norm(hidden), w_out, preferred_element_type=jnp.float32)

    row_spec = P('dp', 'sp', None)
    pos_spec = P(('dp', 'sp'), None)
    arg_specs = (row_spec, P('dp', 'sp'), pos_spec, pos_spec) + (P(),) * 13
    return jax.shard_map(local_program, mesh=mesh, in_specs=arg_specs, out_specs=row_spec, check_vma=False)
```

```python
import functools

import jax
import jax.numpy as jnp
from jax import lax
from jax.experimental import pallas as pl
from jax.experimental.pallas import tpu as pltpu
from jax.sharding import PartitionSpec as P

KEEP_DIV = 8
ENC_PIECES = 2
DEC_PIECES = 2
MESH = pl.DeviceIdType.MESH
LOG2E = 1.4426950408889634
NT = (((1,), (1,)), ((), ()))
TN = (((0,), (0,)), ((), ()))


def layer_norm(hidden):
    hid_f32 = hidden.astype(jnp.float32)
    centred = hid_f32 - jnp.mean(hid_f32, axis=-1, keepdims=True)
    row_var = jnp.mean(centred * centred, axis=-1, keepdims=True)
    return (centred * lax.rsqrt(row_var + 1e-6)).astype(jnp.bfloat16)


def gelu(x):
    return 0.5 * x * (1.0 + lax.erf(x * 0.7071067811865476))


def fdot(lhs, rhs, dims=(((1,), (0,)), ((), ()))):
    return lax.dot_general(lhs, rhs, dims, preferred_element_type=jnp.float32)


class RingGather:
    def __init__(self, n_chips, pieces, buf, send, recv):
        self.n, self.pieces, self.buf, self.send, self.recv = n_chips, pieces, buf, send, recv
        self.rows = buf.shape[3] // pieces
        me = lax.axis_index('sp')
        size = 2 * n_chips
        self.right = lax.rem(me + 2, size)
        self.left = lax.rem(me + size - 2, size)
        self.mate = me + 1 - 2 * lax.rem(me, 2)
        self.arrivals = pieces * (n_chips // 2 - 1) + pieces // 2

    def barrier(self):
        sem = pltpu.get_barrier_semaphore()
        for peer in (self.left, self.right, self.mate):
            pl.semaphore_signal(sem, inc=1, device_id={'sp': peer}, device_id_type=MESH)
        pl.semaphore_wait(sem, 3)

    def copy(self, phase, kind, step, piece):
        if kind == 2:
            src, dst, dst_core, peer = step, step, 1, self.mate
        elif kind == 0:
            src, dst, dst_core, peer = step, step + 1, 0, self.right
        else:
            src, dst, dst_core, peer = lax.rem(self.n - step, self.n), self.n - 1 - step, 0, self.left
        rows = pl.ds(pl.multiple_of(piece * self.rows, self.rows), self.rows)
        return pltpu.make_async_remote_copy(
            src_ref=self.buf.at[phase, src, 0, rows], dst_ref=self.buf.at[phase, dst, dst_core, rows],
            send_sem=self.send.at[phase, kind, step, piece], recv_sem=self.recv.at[phase, kind, step, piece],
            device_id={'sp': peer}, device_id_type=MESH)

    def begin(self, phase):
        for piece in range(self.pieces):
            self.copy(phase, 0, 0, piece).start()
            self.copy(phase, 1, 0, self.pieces - 1 - piece).start()
            self.copy(phase, 2, 0, piece).start()

    def relay(self, phase, k):
        step = k // self.pieces
        p_right = lax.rem(k, self.pieces)
        p_left = self.pieces - 1 - p_right
        self.copy(phase, 0, step, p_right).wait_recv()
        pl.when(k < self.arrivals - self.pieces)(lambda: self.copy(phase, 0, step + 1, p_right).start())
        self.copy(phase, 2, step + 1, p_right).start()
        self.copy(phase, 1, step, p_left).wait_recv()
        pl.when(k < self.arrivals - self.pieces)(lambda: self.copy(phase, 1, step + 1, p_left).start())
        self.copy(phase, 2, self.n - 1 - step, p_left).start()

    def relay_range(self, phase, low, high):
        lax.fori_loop(low, high, lambda k, carry: (self.relay(phase, k), carry)[1], 0)

    def take(self, phase, slot):
        for piece in range(self.pieces):
            self.copy(phase, 2, slot, piece).wait_recv()

    def drain(self, phases):
        def per_slot(i, carry):
            slot = lax.rem(i // self.pieces, self.n)
            self.copy(i // (self.pieces * self.n), 2, slot, lax.rem(i, self.pieces)).wait_send()
            return carry

        def per_hop(i, carry):
            phase, k = i // self.arrivals, lax.rem(i, self.arrivals)
            self.copy(phase, 0, k // self.pieces, lax.rem(k, self.pieces)).wait_send()
            self.copy(phase, 1, k // self.pieces, self.pieces - 1 - lax.rem(k, self.pieces)).wait_send()
            return carry

        lax.fori_loop(0, phases * self.pieces * self.n, per_slot, 0)
        lax.fori_loop(0, phases * self.arrivals, per_hop, 0)


def decoder_kernel(n_chips, n_heads, u_ref, wqkv_hbm, wproj_hbm, wup_hbm, wdown_hbm, state,
                   gath, k_ref, vt_ref, s_even, s_odd, m_ref, qm_ref, ot_ref, acc_ref, sum_ref, top_ref, wqkv, wproj, wup, wdown, send, recv, wsem):
    n_clips, rows, width = u_ref.shape
    n_layers = wproj.shape[0]
    phases = n_layers * n_clips
    head_dim = width // n_heads
    lane_heads = qm_ref.shape[1] // head_dim
    chunk = 2 * rows
    scale = head_dim ** -0.5 * LOG2E
    s_both = (s_even, s_odd)
    ring = RingGather(n_chips, DEC_PIECES, gath, send, recv)

    weights = [pltpu.make_async_copy(src, dst, wsem.at[i]) for i, (src, dst) in enumerate(
        ((wqkv_hbm, wqkv), (wproj_hbm, wproj), (wup_hbm, wup), (wdown_hbm, wdown)))]
    for copy in weights:
        copy.start()
    for clip in range(n_clips):
        state[clip] = u_ref[clip]
        gath[clip, 0, 0] = layer_norm(u_ref[clip])
    qm_ref[...] = jnp.zeros_like(qm_ref)
    ring.barrier()
    ring.begin(0)
    for copy in weights:
        copy.wait()

    def scores(head, base, j, slot, top):
        group = head // lane_heads
        keys = k_ref[base + j, :, pl.ds(pl.multiple_of(group * qm_ref.shape[1], qm_ref.shape[1]), qm_ref.shape[1])]
        s = fdot(keys, qm_ref[head]).reshape(chunk // 8, 8, rows)
        s_both[slot][j] = s
        return jnp.maximum(top, jnp.max(s, axis=0))

    def set_top(slot, top):
        m_ref[slot] = jnp.broadcast_to(jnp.max(top, axis=0, keepdims=True), top.shape)

    def values(head, base, j, slot, total, acc):
        e = jnp.exp2((s_both[slot][j] - m_ref[slot][None]) * scale)
        vt = vt_ref[base + j, pl.ds(pl.multiple_of(head * head_dim, head_dim), head_dim), :]
        return total + jnp.sum(e, axis=0), acc + fdot(vt, e.reshape(chunk, rows).astype(jnp.bfloat16))

    def head_rows(head):
        return pl.ds(pl.multiple_of(head * head_dim, head_dim), head_dim)

    def put_out(head, slot, total, acc):
        ot_ref[head_rows(head), :] = (acc * (1.0 / jnp.sum(total, axis=0, keepdims=True))).astype(jnp.bfloat16)

    def put_first(head, slot, total, acc):
        top_ref[head] = m_ref[slot]
        sum_ref[head] = total
        acc_ref[head_rows(head), :] = acc

    def put_second(head, slot, total, acc):
        old, new = top_ref[head], m_ref[slot]
        top = jnp.maximum(old, new)
        keep_old, keep_new = jnp.exp2((old - top) * scale), jnp.exp2((new - top) * scale)
        put_out(head, slot, sum_ref[head] * keep_old + total * keep_new,
                acc_ref[head_rows(head), :] * keep_old[0:1] + acc * keep_new[0:1])

    lowest = jnp.full((8, rows), -jnp.inf, jnp.float32)
    none = jnp.zeros((8, rows), jnp.float32)
    zero = jnp.zeros((head_dim, rows), jnp.float32)
    half_chips = n_chips // 2
    assert ring.arrivals == 7 and n_heads == 16

    def sweep(base, count, put, between):
        top = lowest
        for j in range(count):
            top = scores(0, base, j, 0, top)
        set_top(0, top)

        def head_step(head, now, last=False):
            top, total, acc = lowest, none, zero
            for j in range(count):
                if not last:
                    top = scores(head + 1, base, j, 1 - now, top)
                total, acc = values(head, base, j, now, total, acc)
            if not last:
                set_top(1 - now, top)
            put(head, now, total, acc)

        def head_pair(pair, carry):
            between(pair)
            head_step(2 * pair, 0)
            head_step(2 * pair + 1, 1)
            return carry

        lax.fori_loop(0, n_heads // 2 - 1, head_pair, 0)
        between(jnp.int32(n_heads // 2 - 1))
        head_step(n_heads - 2, 0)
        head_step(n_heads - 1, 1, last=True)

    def queries(phase, layer):
        qt = fdot(wqkv[layer, 0], gath[phase, 0, 0], NT).astype(jnp.bfloat16)
        for head in range(n_heads):
            at = (head % lane_heads) * head_dim
            qm_ref[head, at:at + head_dim, :] = qt[head * head_dim:(head + 1) * head_dim]

    def project(phase, layer, i):
        r = jnp.where(lax.rem(i, 2) == 1, (i + 1) // 2, lax.rem(n_chips - i // 2, n_chips))
        ring.take(phase, r)
        a = gath[phase, r].reshape(chunk, width)
        k_ref[i] = fdot(a, wqkv[layer, 1], NT).astype(jnp.bfloat16)
        vt_ref[i] = fdot(wqkv[layer, 2], a, NT).astype(jnp.bfloat16)

    def complete(phase, layer, clip):
        mid = (state[clip].astype(jnp.float32) + fdot(ot_ref[...], wproj[layer], TN)).astype(jnp.bfloat16)
        normed = layer_norm(mid)
        down = mid.astype(jnp.float32)
        for f in range(0, wup.shape[2], width):
            act = gelu(fdot(normed, wup[layer, :, f:f + width])).astype(jnp.bfloat16)
            down = down + fdot(act, wdown[layer, f:f + width, :])
        new = down.astype(jnp.bfloat16)
        state[clip] = new

        @pl.when(phase + n_clips < phases)
        def _():
            gath[phase + n_clips, 0, 0] = layer_norm(new)

        @pl.when(phase + n_clips >= phases)
        def _():
            state[clip] = layer_norm(new)


    def opening(i, carry):
        pl.when(lax.rem(i, 2) == 1)(lambda: ring.relay_range(0, i - 1, i + 1))
        project(0, 0, i)
        return carry

    def rest(i, carry):
        project(0, 0, i)
        return carry

    def between_first(pair):
        pl.when((pair == 1) | (pair == 3) | (pair == 5))(lambda: ring.relay(0, half_chips + pair // 2))
        pl.when(pair == 3)(lambda: ring.begin(1))

    def between_second(pair):
        pl.when((pair == 0) | (pair == 3) | (pair == 5) | (pair == 7))(lambda: ring.relay(1, pair // 2))

    queries(0, 0)
    lax.fori_loop(0, half_chips, opening, 0)
    sweep(0, half_chips, put_first, between_first)
    lax.fori_loop(half_chips, n_chips, rest, 0)
    sweep(half_chips, half_chips, put_second, between_second)
    complete(0, 0, 0)
    ring.relay(1, half_chips)

    def phase_body(phase, carry):
        clip = lax.rem(phase, n_clips)
        layer = phase // n_clips
        more = phase + 1 < phases
        pl.when(more & (phase > 1))(lambda: ring.begin(phase + 1))

        def project_all(i, carry):
            pl.when((phase == 1) & (i == 5))(lambda: ring.relay(phase, 5))
            pl.when((phase == 1) & (i == 7))(lambda: ring.relay(phase, 6))
            pl.when(more & (phase == 1) & (i == 6))(lambda: ring.begin(phase + 1))
            project(phase, layer, i)
            return carry

        def between(pair):
            late = (pair > 2).astype(jnp.int32) + (pair > 5).astype(jnp.int32)
            pl.when(more & (pair != 2) & (pair != 5))(lambda: ring.relay(phase + 1, pair - late))

        lax.fori_loop(0, n_chips, project_all, 0)
        queries(phase, layer)
        sweep(0, n_chips, put_out, between)
        complete(phase, layer, clip)
        pl.when(more)(lambda: ring.relay(phase + 1, ring.arrivals - 1))
        return carry

    lax.fori_loop(1, phases, phase_body, 0)
    ring.drain(phases)


def run_decoder(n_chips, u, w_qkv, w_proj, w_up, w_down):
    n_clips, rows, width = u.shape
    n_layers, _, _, n_heads, head_dim = w_qkv.shape
    phases = n_layers * n_clips
    w_qkv = jnp.transpose(w_qkv, (0, 2, 3, 4, 1)).reshape(n_layers, 3, width, width)
    w_proj = w_proj.reshape(n_layers, width, width)
    mlp = w_up.shape[2]
    bf = jnp.bfloat16
    vmem, hbm = pl.BlockSpec(memory_space=pltpu.VMEM), pl.BlockSpec(memory_space=pl.ANY)
    keys = 2 * n_chips * rows
    return pl.pallas_call(
        functools.partial(decoder_kernel, n_chips, n_heads),
        out_shape=jax.ShapeDtypeStruct(u.shape, bf),
        in_specs=[vmem, hbm, hbm, hbm, hbm],
        out_specs=vmem,
        scratch_shapes=[
            pltpu.VMEM((phases, n_chips, 2, rows, width), bf),
            pltpu.VMEM((n_chips, 2 * rows, width), bf),
            pltpu.VMEM((n_chips, width, 2 * rows), bf),
            pltpu.VMEM((n_chips, rows // 4, 8, rows), jnp.float32),
            pltpu.VMEM((n_chips, rows // 4, 8, rows), jnp.float32),
            pltpu.VMEM((2, 8, rows), jnp.float32),
            pltpu.VMEM((n_heads, 256, rows), bf),
            pltpu.VMEM((width, rows), bf),
            pltpu.VMEM((width, rows), jnp.float32),
            pltpu.VMEM((n_heads, 8, rows), jnp.float32),
            pltpu.VMEM((n_heads, 8, rows), jnp.float32),
            pltpu.VMEM((n_layers, 3, width, width), bf),
            pltpu.VMEM((n_layers, width, width), bf),
            pltpu.VMEM((n_layers, width, mlp), bf),
            pltpu.VMEM((n_layers, mlp, width), bf),
            pltpu.SemaphoreType.DMA((phases, 3, n_chips, DEC_PIECES)),
            pltpu.SemaphoreType.DMA((phases, 3, n_chips, DEC_PIECES)),
            pltpu.SemaphoreType.DMA((4,)),
        ],
        compiler_params=pltpu.CompilerParams(collective_id=1, has_side_effects=True, vmem_limit_bytes=60 * 1024 * 1024),
        cost_estimate=pl.CostEstimate(flops=phases * n_heads * keys * rows * 2 * (256 + head_dim), bytes_accessed=16 * 1024 * 1024, transcendentals=phases * n_heads * keys * rows),
        name='decoder',
    )(u, w_qkv, w_proj, w_up, w_down)


def encoder_kernel(n_chips, n_heads, patches_hbm, mask_ref, epos_hbm, dpos_hbm, wpe_hbm, bias_ref, wqkv_hbm, wproj_hbm,
                   wup_hbm, wdown_hbm, wed_hbm, token_ref, u_ref,
                   patches, epos, dpos, wpe, wqkv, wproj, wup, wdown, wed,
                   gath, kvt, q_ref, o_ref, hid, mx_ref, sel_ref, shift_ref, emb_ref, place_ref, edge_ref, z_ref, count_ref,
                   send, recv, csend, crecv, esend, erecv, fsem, wsem):
    n_clips, tokens, _ = u_ref.shape
    n_layers, width = wproj.shape[0], wproj.shape[1]
    size = 2 * n_chips
    keep = hid.shape[0] // n_clips
    half = keep // 2
    slots = 2 * keep
    head_dim = width // n_heads
    lanes = 256
    pack = lanes // head_dim
    scale = head_dim ** -0.5 * LOG2E
    bf, f32 = jnp.bfloat16, jnp.float32
    ring = RingGather(n_chips, ENC_PIECES, gath, send, recv)
    me = lax.axis_index('sp')

    fetch = [pltpu.make_async_copy(src, dst, fsem.at[i]) for i, (src, dst) in enumerate(
        ((patches_hbm, patches), (wpe_hbm, wpe), (epos_hbm, epos), (dpos_hbm, dpos), (wed_hbm, wed)))]
    for copy in fetch:
        copy.start()

    def layer_copy(layer, i):
        src = (wqkv_hbm, wproj_hbm, wup_hbm, wdown_hbm)[i].at[layer]
        dst = (wqkv.at[layer], wproj.at[layer], wup, wdown)[i]
        return pltpu.make_async_copy(src, dst, wsem.at[layer, i])

    sem = pltpu.get_barrier_semaphore()

    def greet(t, carry):
        pl.semaphore_signal(sem, inc=1, device_id={'sp': lax.rem(me + t, size)}, device_id_type=MESH)
        return carry

    lax.fori_loop(1, size, greet, 0)

    row_id = lax.broadcasted_iota(jnp.int32, (slots, tokens), 0).astype(f32)
    earlier = (lax.broadcasted_iota(jnp.int32, (tokens, tokens), 0)
               < lax.broadcasted_iota(jnp.int32, (tokens, tokens), 1)).astype(f32).astype(bf)
    masks = [jnp.broadcast_to(mask_ref[c:c + 1, :].astype(f32), (8, tokens)) for c in range(n_clips)]
    line = lax.broadcasted_iota(jnp.int32, (8, 128), 0)
    mine = jnp.zeros((8, 128), f32)
    occupied = []
    for c in range(n_clips):
        mine = jnp.where(line == c, jnp.sum(masks[c], axis=1, keepdims=True), mine)
        rank = fdot(masks[c].astype(bf), earlier)
        sel = jnp.where((row_id == rank[0:1]) & (masks[c][0:1] > 0.5), 1.0, 0.0)
        occupied.append(jnp.sum(sel, axis=1, keepdims=True))
        sel_ref[c] = sel.astype(bf)
    count_ref[me] = mine
    pl.semaphore_wait(sem, size - 1)

    def count_copy(t):
        return pltpu.make_async_remote_copy(
            src_ref=count_ref.at[me], dst_ref=count_ref.at[me], send_sem=csend.at[t], recv_sem=crecv.at[t],
            device_id={'sp': lax.rem(me + t, size)}, device_id_type=MESH)

    def count_from(t):
        src = lax.rem(me + size - t, size)
        return pltpu.make_async_remote_copy(
            src_ref=count_ref.at[src], dst_ref=count_ref.at[src], send_sem=csend.at[t], recv_sem=crecv.at[t],
            device_id={'sp': lax.rem(me + t, size)}, device_id_type=MESH)

    lax.fori_loop(1, size, lambda t, carry: (count_copy(t).start(), carry)[1], 0)
    for copy in fetch[:3]:
        copy.wait()
    for i in range(4):
        layer_copy(0, i).start()
    for layer in range(1, n_layers):
        for i in range(2):
            layer_copy(layer, i).start()

    for c in range(n_clips):
        mx_ref[c * slots:(c + 1) * slots] = fdot(sel_ref[c], patches[c]).astype(bf)
    embedded = fdot(mx_ref[...], wpe[...])
    bias = bias_ref[...].astype(f32).reshape(1, width)
    for c in range(n_clips):
        emb_ref[c] = (embedded[c * slots:(c + 1) * slots] + occupied[c] * bias + fdot(sel_ref[c], epos[...])).astype(bf)

    lax.fori_loop(1, size, lambda t, carry: (count_from(t).wait_recv(), carry)[1], 0)
    source = lax.broadcasted_iota(jnp.int32, (size, 8, 128), 0)
    offset = (half - me * keep).astype(f32) + jnp.sum(jnp.where(source < me, count_ref[...], 0.0), axis=0)
    apart = (lax.broadcasted_iota(jnp.int32, (slots, slots), 0) - lax.broadcasted_iota(jnp.int32, (slots, slots), 1)).astype(f32)
    for c in range(n_clips):
        shift_ref[c] = jnp.where(apart == offset[c:c + 1, :slots], 1.0, 0.0).astype(bf)
        place_ref[c] = fdot(shift_ref[c], emb_ref[c]).astype(bf)

    after, before = lax.rem(me + 1, size), lax.rem(me + size - 1, size)

    def edge_copy(i, src, dst, peer):
        return pltpu.make_async_remote_copy(src_ref=src, dst_ref=dst, send_sem=esend.at[i], recv_sem=erecv.at[i],
                                            device_id={'sp': peer}, device_id_type=MESH)

    edges = [edge_copy(0, place_ref.at[:, pl.ds(slots - half, half)], edge_ref.at[0], after),
             edge_copy(1, place_ref.at[:, pl.ds(0, half)], edge_ref.at[1], before)]
    for copy in edges:
        copy.start()
    for copy in edges:
        copy.wait_recv()
    for c in range(n_clips):
        for i in range(2):
            hid[c * keep + i * half:c * keep + (i + 1) * half] = (
                place_ref[c, half + i * half:half + (i + 1) * half].astype(f32) + edge_ref[i, c].astype(f32)).astype(bf)
    gath[0, 0, 0] = layer_norm(hid[...])

    block = (lax.broadcasted_iota(jnp.int32, (pack * keep, lanes), 0) // keep
             == lax.broadcasted_iota(jnp.int32, (pack * keep, lanes), 1) // head_dim).astype(f32)
    block_bf = block.astype(bf)
    order = [0]
    for i in range(1, n_chips // 2):
        order += [i, n_chips - i]
    order.append(n_chips // 2)
    n_parts = 2
    part = n_chips // n_parts
    part_keys = part * 2 * keep

    def layer_body(layer, carry):
        ring.begin(layer)
        layer_copy(layer, 0).wait()
        q_ref[...] = fdot(gath[layer, 0, 0], wqkv[layer, :width], NT).astype(bf)
        for i in range(n_parts):
            picked = order[i * part:(i + 1) * part]
            edge = ring.pieces * (n_chips // 4)
            ready = ring.arrivals if i == n_parts - 1 else edge
            done = 0 if i == 0 else edge + ring.pieces // 2 + 1
            ring.relay_range(layer, done, ready)
            for slot in picked:
                ring.take(layer, slot)
            for c in range(n_clips):
                if i == 0 and c == 1:
                    ring.relay_range(layer, edge, edge + ring.pieces // 2 + 1)
                a = jnp.concatenate([gath[layer, slot, :, c * keep:(c + 1) * keep].reshape(2 * keep, width) for slot in picked], axis=0)
                kvt[c, :, i * part_keys:(i + 1) * part_keys] = fdot(wqkv[layer, width:], a, NT).astype(bf)

        for c in range(n_clips):
            for g in range(width // lanes):
                at = slice(g * lanes, (g + 1) * lanes)
                q = q_ref[c * keep:(c + 1) * keep, at]
                s = fdot(jnp.concatenate([q] * pack, axis=0) * block_bf, kvt[c, at, :])
                e = jnp.exp2((s - jnp.max(s, axis=1, keepdims=True)) * scale)
                p = (e * (1.0 / jnp.sum(e, axis=1, keepdims=True))).astype(bf)
                o = fdot(p, kvt[c, width + g * lanes:width + (g + 1) * lanes, :], NT) * block
                total = o[:keep]
                for h in range(1, pack):
                    total = total + o[h * keep:(h + 1) * keep]
                o_ref[c * keep:(c + 1) * keep, at] = total.astype(bf)

        layer_copy(layer, 1).wait()
        mid = (hid[...].astype(f32) + fdot(o_ref[...], wproj[layer])).astype(bf)
        normed = layer_norm(mid)
        down = mid.astype(f32)
        layer_copy(layer, 2).wait()
        layer_copy(layer, 3).wait()
        for f in range(0, wup.shape[1], width):
            act = gelu(fdot(normed, wup[:, f:f + width])).astype(bf)
            down = down + fdot(act, wdown[f:f + width, :])
        new = down.astype(bf)
        hid[...] = new

        @pl.when(layer + 1 < n_layers)
        def _():
            for i in (2, 3):
                layer_copy(layer + 1, i).start()
            gath[layer + 1, 0, 0] = layer_norm(new)

        return carry

    lax.fori_loop(0, n_layers, layer_body, 0)

    for copy in fetch[3:]:
        copy.wait()
    z = fdot(layer_norm(hid[...]), wed[...]).astype(bf)
    for c in range(n_clips):
        z_ref[c, half:half + keep] = z[c * keep:(c + 1) * keep]
    z_edges = [edge_copy(2, z_ref.at[:, pl.ds(keep, half)], z_ref.at[:, pl.ds(0, half)], after),
               edge_copy(3, z_ref.at[:, pl.ds(half, half)], z_ref.at[:, pl.ds(half + keep, half)], before)]
    for copy in z_edges:
        copy.start()
    first_line = lax.broadcasted_iota(jnp.int32, (8, tokens), 0) == 0
    token = jnp.broadcast_to(token_ref[...].astype(f32).reshape(1, token_ref.shape[0]), (8, token_ref.shape[0])).astype(bf)
    hidden_part = [fdot(jnp.where(first_line, 1.0 - m, 0.0).astype(bf), token, TN) for m in masks]
    for copy in z_edges:
        copy.wait_recv()
    for c in range(n_clips):
        own = fdot(shift_ref[c], z_ref[c], TN).astype(bf)
        u_ref[c] = (fdot(sel_ref[c], own, TN) + hidden_part[c] + dpos[...].astype(f32)).astype(bf)

    lax.fori_loop(1, size, lambda t, carry: (count_copy(t).wait_send(), carry)[1], 0)
    for copy in edges + z_edges:
        copy.wait_send()
    ring.drain(n_layers)


def run_encoder(n_chips, patches, mask, enc_pos, dec_pos, w_pe, b_pe, w_qkv, w_proj, w_up, w_down, w_ed, token):
    n_clips, tokens, patch = patches.shape
    n_layers, width, _, n_heads, head_dim = w_qkv.shape
    mlp, out_width = w_up.shape[2], w_ed.shape[1]
    keep = tokens // KEEP_DIV
    rows, slots = n_clips * keep, 2 * keep
    bf, f32 = jnp.bfloat16, jnp.float32
    w_qkv = jnp.transpose(w_qkv, (0, 2, 3, 4, 1)).reshape(n_layers, 3 * width, width)
    w_proj = w_proj.reshape(n_layers, width, width)
    vmem, hbm = pl.BlockSpec(memory_space=pltpu.VMEM), pl.BlockSpec(memory_space=pl.ANY)
    dma = pltpu.SemaphoreType.DMA
    keys = 2 * n_chips * keep
    flops = 2 * n_layers * rows * width * (4 * width + 2 * mlp) + 4 * n_layers * keys * n_clips * width * width
    return pl.pallas_call(
        functools.partial(encoder_kernel, n_chips, n_heads),
        out_shape=jax.ShapeDtypeStruct((n_clips, tokens, out_width), bf),
        in_specs=[hbm, vmem, hbm, hbm, hbm, vmem, hbm, hbm, hbm, hbm, hbm, vmem],
        out_specs=vmem,
        scratch_shapes=[
            pltpu.VMEM(patches.shape, bf), pltpu.VMEM(enc_pos.shape, bf), pltpu.VMEM(dec_pos.shape, bf),
            pltpu.VMEM(w_pe.shape, bf), pltpu.VMEM(w_qkv.shape, bf), pltpu.VMEM(w_proj.shape, bf),
            pltpu.VMEM(w_up.shape[1:], bf), pltpu.VMEM(w_down.shape[1:], bf), pltpu.VMEM(w_ed.shape, bf),
            pltpu.VMEM((n_layers, n_chips, 2, rows, width), bf),
            pltpu.VMEM((n_clips, 2 * width, keys), bf),
            pltpu.VMEM((rows, width), bf), pltpu.VMEM((rows, width), bf), pltpu.VMEM((rows, width), bf),
            pltpu.VMEM((n_clips * slots, patch), bf),
            pltpu.VMEM((n_clips, slots, tokens), bf), pltpu.VMEM((n_clips, slots, slots), bf),
            pltpu.VMEM((n_clips, slots, width), bf), pltpu.VMEM((n_clips, slots, width), bf),
            pltpu.VMEM((2, n_clips, keep // 2, width), bf), pltpu.VMEM((n_clips, slots, out_width), bf),
            pltpu.VMEM((2 * n_chips, 8, 128), f32),
            dma((n_layers, 3, n_chips, ENC_PIECES)), dma((n_layers, 3, n_chips, ENC_PIECES)),
            dma((2 * n_chips,)), dma((2 * n_chips,)), dma((4,)), dma((4,)), dma((5,)), dma((n_layers, 4)),
        ],
        compiler_params=pltpu.CompilerParams(collective_id=2, has_side_effects=True, vmem_limit_bytes=60 * 1024 * 1024),
        cost_estimate=pl.CostEstimate(flops=flops, bytes_accessed=56 * 1024 * 1024, transcendentals=0),
        name='encoder',
    )(patches, mask, enc_pos, dec_pos, w_pe, b_pe, w_qkv, w_proj, w_up, w_down, w_ed, token)


def solution(mesh):
    n_chips = mesh.shape['sp'] // 2

    def local_program(patches, vis_mask, enc_pos, dec_pos, w_pe, b_pe, enc_qkv, enc_proj, enc_up, enc_down, w_ed, mask_token, dec_qkv, dec_proj, dec_up, dec_down, w_out):
        hidden = run_encoder(n_chips, patches, vis_mask, enc_pos, dec_pos, w_pe, b_pe, enc_qkv, enc_proj, enc_up, enc_down, w_ed, mask_token)
        hidden = run_decoder(n_chips, hidden, dec_qkv, dec_proj, dec_up, dec_down)
        return jnp.einsum('cne,ep->cnp', hidden, w_out, preferred_element_type=jnp.float32)

    row_spec = P('dp', 'sp', None)
    pos_spec = P(('dp', 'sp'), None)
    arg_specs = (row_spec, P('dp', 'sp'), pos_spec, pos_spec) + (P(),) * 13
    return jax.shard_map(local_program, mesh=mesh, in_specs=arg_specs, out_specs=row_spec, check_vma=False)
```
